32 devices in a mesh: dp: 4 (over x, y), tp: 8 (over z, core).
Axes of the slice: x: 2, y: 2, z: 4, core: 2. Of those that a mesh axis runs over, the one named last changes fastest.
Arguments:
- x_saved: bfloat16 [8, 2048, 1024], P('dp'), parts along dimension 0
- h1_saved: bfloat16 [8, 2048, 1024], P('dp'), parts along dimension 0
- grad_y: bfloat16 [8, 2048, 1024], P('dp'), parts along dimension 0
- mean_one: float32 [8, 2048], P('dp'), parts along dimension 0
- rstd_one: float32 [8, 2048], P('dp'), parts along dimension 0
- mean_two: float32 [8, 2048], P('dp'), parts along dimension 0
- rstd_two: float32 [8, 2048], P('dp'), parts along dimension 0
- gain_one: bfloat16 [1024], replicated
- gain_two: bfloat16 [1024], replicated
- w_qkv: bfloat16 [1024, 16, 3, 64], P(None, 'tp')
- w_out: bfloat16 [16, 64, 1024], P('tp')
- w_up: bfloat16 [1024, 4096], P(None, 'tp')
- w_down: bfloat16 [4096, 1024], P('tp')
Outputs:
- output 1: bfloat16 [8, 2048, 1024], P('dp'), parts along dimension 0
- output 2: bfloat16 [4096, 16, 3, 64], P('dp', 'tp'), parts along dimension 0
- output 3: bfloat16 [64, 64, 1024], P(('dp', 'tp')), parts along dimension 0
- output 4: bfloat16 [4096, 4096], P('dp', 'tp'), parts along dimension 0
- output 5: bfloat16 [16384, 1024], P(('dp', 'tp')), parts along dimension 0
There are 4 independent parts. The reference program is written for one: setup_inputs(seed, part) draws one part's arguments, and reference() takes and returns one part's arrays. A program takes and returns all parts, laid end to end along the dimension named above; an argument that names none is the same for every part.
All inputs are finite; a program needn't handle non-finite values.
Results may differ from the reference program's by a relative error of at most 0.0176086.
Values are sent between devices in bfloat16 or wider.
A program may use at most 1 GiB of HBM per device.

```python
import math
import jax
import jax.numpy as jnp
from jax import lax
from functools import partial

HIDDEN = 1024
NUM_HEADS = 16
FFN_DIM = 4096
SEQ_LEN = 2048
MICROBATCHES = 2

HEAD_DIM = HIDDEN // NUM_HEADS
TOKENS = MICROBATCHES * SEQ_LEN
GELU_C = 0.7978845608028654
GELU_A = 0.044715
NORM_EPS = 1e-5
wide_dot = partial(jnp.dot, preferred_element_type=jnp.float32)


def row_stats(acts):
    row_vals = acts.astype(jnp.float32)
    row_mean = jnp.mean(row_vals, axis=-1)
    row_var = jnp.mean(jnp.square(row_vals - row_mean[..., None]), axis=-1)
    return row_mean, lax.rsqrt(row_var + NORM_EPS)


def setup_inputs(seed: int = 0, part: int = 0) -> dict:
    shared_key, part_root = jax.random.split(jax.random.key(seed))
    act_keys = jax.random.split(jax.random.fold_in(part_root, part), 7)
    weight_keys = jax.random.split(shared_key, 6)
    act_shape = (MICROBATCHES, SEQ_LEN, HIDDEN)
    row_shape = (MICROBATCHES, SEQ_LEN, 1)
    x_saved = (jax.random.normal(act_keys[0], row_shape)
               + jax.random.uniform(act_keys[1], row_shape, minval=0.5, maxval=2.0)
               * jax.random.normal(act_keys[2], act_shape)).astype(jnp.bfloat16)
    h1_saved = (0.5 * jax.random.normal(act_keys[3], row_shape)
                + jax.random.uniform(act_keys[4], row_shape, minval=0.4, maxval=1.2)
                * jax.random.normal(act_keys[5], act_shape)).astype(jnp.bfloat16)
    grad_y = jax.random.normal(act_keys[6], act_shape).astype(jnp.bfloat16)
    mean_one, rstd_one = row_stats(x_saved)
    mean_two, rstd_two = row_stats(h1_saved)
    gain_one = jax.random.uniform(weight_keys[0], (HIDDEN,), minval=0.5, maxval=1.5).astype(jnp.bfloat16)
    gain_two = jax.random.uniform(weight_keys[1], (HIDDEN,), minval=0.5, maxval=1.5).astype(jnp.bfloat16)
    qk_gain = math.sqrt(math.log(SEQ_LEN))
    head_gain = jnp.array([qk_gain, 1.0, 1.0], dtype=jnp.float32)[:, None]
    w_qkv = (jax.random.normal(weight_keys[2], (HIDDEN, NUM_HEADS, 3, HEAD_DIM)) * head_gain
             * HIDDEN ** -0.5).astype(jnp.bfloat16)
    w_out = (jax.random.normal(weight_keys[3], (NUM_HEADS, HEAD_DIM, HIDDEN)) * HIDDEN ** -0.5).astype(jnp.bfloat16)
    w_up = (jax.random.normal(weight_keys[4], (HIDDEN, FFN_DIM)) * HIDDEN ** -0.5).astype(jnp.bfloat16)
    w_down = (jax.random.normal(weight_keys[5], (FFN_DIM, HIDDEN)) * FFN_DIM ** -0.5).astype(jnp.bfloat16)
    return {'x_saved': x_saved, 'h1_saved': h1_saved, 'grad_y': grad_y,
            'mean_one': mean_one, 'rstd_one': rstd_one, 'mean_two': mean_two, 'rstd_two': rstd_two,
            'gain_one': gain_one, 'gain_two': gain_two,
            'w_qkv': w_qkv, 'w_out': w_out, 'w_up': w_up, 'w_down': w_down}


def gelu_tanh(pre_act):
    inner_arg = GELU_C * (pre_act + GELU_A * pre_act * pre_act * pre_act)
    return 0.5 * pre_act * (1.0 + jnp.tanh(inner_arg))


def gelu_slope(pre_act):
    inner_arg = GELU_C * (pre_act + GELU_A * pre_act * pre_act * pre_act)
    tanh_val = jnp.tanh(inner_arg)
    return (0.5 * (1.0 + tanh_val)
            + 0.5 * pre_act * (1.0 - tanh_val * tanh_val) * GELU_C * (1.0 + 3.0 * GELU_A * pre_act * pre_act))


def norm_backward(grad_norm, xhat, gain, rstd):
    scaled = grad_norm * gain.astype(jnp.float32)
    mean_scaled = jnp.mean(scaled, axis=-1, keepdims=True)
    mean_cross = jnp.mean(scaled * xhat, axis=-1, keepdims=True)
    return rstd[..., None] * (scaled - mean_scaled - xhat * mean_cross)


def head_backward(operands):
    q_heads, k_heads, v_heads, grad_o = operands
    score_scale = HEAD_DIM ** -0.5
    scores = wide_dot(q_heads, k_heads.T) * score_scale
    causal = jnp.arange(SEQ_LEN)[:, None] >= jnp.arange(SEQ_LEN)[None, :]
    attn_prob = jax.nn.softmax(jnp.where(causal, scores, -1e30), axis=-1)
    prob_bf16 = attn_prob.astype(jnp.bfloat16)
    attn_out = wide_dot(prob_bf16, v_heads).astype(jnp.bfloat16)
    grad_v = wide_dot(prob_bf16.T, grad_o).astype(jnp.bfloat16)
    grad_p = wide_dot(grad_o, v_heads.T)
    row_dot = jnp.sum(attn_prob * grad_p, axis=-1, keepdims=True)
    grad_s = (attn_prob * (grad_p - row_dot) * score_scale).astype(jnp.bfloat16)
    grad_q = wide_dot(grad_s, k_heads).astype(jnp.bfloat16)
    grad_k = wide_dot(grad_s.T, q_heads).astype(jnp.bfloat16)
    return attn_out, jnp.stack([grad_q, grad_k, grad_v], axis=1)


def split_heads(rows):
    return rows.reshape(MICROBATCHES, SEQ_LEN, NUM_HEADS, HEAD_DIM).transpose(0, 2, 1, 3).reshape(
        MICROBATCHES * NUM_HEADS, SEQ_LEN, HEAD_DIM)


def reference(x_saved, h1_saved, grad_y, mean_one, rstd_one, mean_two, rstd_two,
              gain_one, gain_two, w_qkv, w_out, w_up, w_down):
    x_rows = x_saved.reshape(TOKENS, HIDDEN)
    h1_rows = h1_saved.reshape(TOKENS, HIDDEN)
    dy_rows = grad_y.reshape(TOKENS, HIDDEN)
    xhat_two = (h1_rows.astype(jnp.float32) - mean_two.reshape(TOKENS, 1)) * rstd_two.reshape(TOKENS, 1)
    norm_two = (xhat_two * gain_two.astype(jnp.float32)).astype(jnp.bfloat16)
    pre_act = wide_dot(norm_two, w_up)
    act_out = gelu_tanh(pre_act).astype(jnp.bfloat16)
    grad_down = wide_dot(act_out.T, dy_rows).astype(jnp.bfloat16)
    grad_pre = (wide_dot(dy_rows, w_down.T) * gelu_slope(pre_act)).astype(jnp.bfloat16)
    grad_up = wide_dot(norm_two.T, grad_pre).astype(jnp.bfloat16)
    grad_norm_two = wide_dot(grad_pre, w_up.T)
    grad_h1 = (dy_rows.astype(jnp.float32)
               + norm_backward(grad_norm_two, xhat_two, gain_two, rstd_two.reshape(TOKENS))).astype(jnp.bfloat16)
    xhat_one = (x_rows.astype(jnp.float32) - mean_one.reshape(TOKENS, 1)) * rstd_one.reshape(TOKENS, 1)
    norm_one = (xhat_one * gain_one.astype(jnp.float32)).astype(jnp.bfloat16)
    qkv_flat = w_qkv.reshape(HIDDEN, 3 * HIDDEN)
    qkv_acts = wide_dot(norm_one, qkv_flat).astype(jnp.bfloat16).reshape(TOKENS, NUM_HEADS, 3, HEAD_DIM)
    grad_o = wide_dot(grad_h1, w_out.reshape(HIDDEN, HIDDEN).T).astype(jnp.bfloat16)
    attn_heads, grad_heads = lax.map(head_backward, (split_heads(qkv_acts[:, :, 0]), split_heads(qkv_acts[:, :, 1]),
                                                     split_heads(qkv_acts[:, :, 2]), split_heads(grad_o)))
    attn_rows = attn_heads.reshape(MICROBATCHES, NUM_HEADS, SEQ_LEN, HEAD_DIM).transpose(0, 2, 1, 3).reshape(
        TOKENS, HIDDEN)
    grad_qkv = grad_heads.reshape(MICROBATCHES, NUM_HEADS, SEQ_LEN, 3, HEAD_DIM).transpose(0, 2, 1, 3, 4).reshape(
        TOKENS, 3 * HIDDEN)
    grad_out_w = wide_dot(attn_rows.T, grad_h1).astype(jnp.bfloat16).reshape(NUM_HEADS, HEAD_DIM, HIDDEN)
    grad_qkv_w = wide_dot(norm_one.T, grad_qkv).astype(jnp.bfloat16).reshape(HIDDEN, NUM_HEADS, 3, HEAD_DIM)
    grad_norm_one = wide_dot(grad_qkv, qkv_flat.T)
    grad_x = (grad_h1.astype(jnp.float32)
              + norm_backward(grad_norm_one, xhat_one, gain_one, rstd_one.reshape(TOKENS))).astype(jnp.bfloat16)
    return grad_x.reshape(MICROBATCHES, SEQ_LEN, HIDDEN), grad_qkv_w, grad_out_w, grad_up, grad_down
```

```python
import functools

import jax
import jax.numpy as jnp
from jax import lax
from jax.experimental import pallas as pl
from jax.experimental.pallas import tpu as pltpu
from jax.sharding import PartitionSpec as P

GELU_C = 0.7978845608028654
GELU_A = 0.044715
F32 = jnp.float32
BF16 = jnp.bfloat16
wide_einsum = functools.partial(jnp.einsum, preferred_element_type=F32)


def gelu_both(pre_act):
    sq = pre_act * pre_act
    tanh_val = jnp.tanh(GELU_C * pre_act * (1.0 + GELU_A * sq))
    half = 0.5 * (1.0 + tanh_val)
    value = pre_act * half
    slope = half + 0.5 * pre_act * (1.0 - tanh_val * tanh_val) * (GELU_C * (1.0 + 3.0 * GELU_A * sq))
    return value, slope


NT = (((1,), (1,)), ((), ()))
NN = (((1,), (0,)), ((), ()))


def dotf(a, b, dims=NN):
    return lax.dot_general(a, b, dims, preferred_element_type=F32)


def attention_kernel(blk, heads, dim, seq, qkv_ref, do_ref, o_ref, dqkv_ref, k_s, v_s, s_s, dp_s, dk_s, dv_s):
    scale = dim ** -0.5
    nb = seq // blk
    for n in range(heads):
        k_s[n] = qkv_ref[n, 1].astype(F32).T.astype(BF16)
        v_s[n] = qkv_ref[n, 2].astype(F32).T.astype(BF16)
        dk_s[n] = jnp.zeros_like(dk_s[n])
        dv_s[n] = jnp.zeros_like(dv_s[n])
    keep = (lax.broadcasted_iota(jnp.int32, (blk, blk), 0) <= lax.broadcasted_iota(jnp.int32, (blk, blk), 1))

    def fold(x, op):
        return op(x.reshape(blk // 8, 8, blk), axis=0)

    for i in range(nb):
        cols = pl.ds(i * blk, blk)
        q_t = [(qkv_ref[n, 0, :, cols].astype(F32) * scale).astype(BF16) for n in range(heads)]
        do_t = [do_ref[n, :, cols] for n in range(heads)]

        def pass_one(j, m, masked):
            rows = pl.ds(pl.multiple_of(j * blk, blk), blk)
            out = []
            for n in range(heads):
                s = dotf(k_s[n, rows], q_t[n])
                if masked:
                    s = jnp.where(keep, s, -1e30)
                s_s[n, rows] = s
                out.append(jnp.maximum(m[n], fold(s, jnp.max)))
            return tuple(out)

        m = tuple(jnp.full((8, blk), -jnp.inf, F32) for _ in range(heads))
        if i:
            m = lax.fori_loop(0, i, lambda j, c: pass_one(j, c, False), m)
        m = pass_one(i, m, True)
        m = [jnp.max(x, axis=0, keepdims=True) for x in m]

        def pass_two(j, carry):
            rows = pl.ds(pl.multiple_of(j * blk, blk), blk)
            out = []
            for n in range(heads):
                l, d = carry[n]
                dp = dotf(v_s[n, rows], do_t[n])
                e = jnp.exp(s_s[n, rows] - m[n])
                s_s[n, rows] = e
                dp_s[n, rows] = dp
                out.append((l + fold(e, jnp.sum), d + fold(e * dp, jnp.sum)))
            return tuple(out)

        zero = jnp.zeros((8, blk), F32)
        stats = lax.fori_loop(0, i + 1, pass_two, tuple((zero, zero) for _ in range(heads)))
        inv = [1.0 / jnp.sum(l, axis=0, keepdims=True) for l, _ in stats]
        dot_row = [jnp.sum(d, axis=0, keepdims=True) * inv[n] for n, (_, d) in enumerate(stats)]

        def pass_three(j, carry):
            rows = pl.ds(pl.multiple_of(j * blk, blk), blk)
            out = []
            for n in range(heads):
                o_t, dq_t = carry[n]
                p = s_s[n, rows] * inv[n]
                pb = p.astype(BF16)
                ds = (p * (dp_s[n, rows] - dot_row[n])).astype(BF16)
                dv_s[n, rows] += dotf(pb, do_t[n], NT)
                dk_s[n, rows] += dotf(ds, q_t[n], NT)
                o_t = o_t + dotf(qkv_ref[n, 2, :, rows], pb)
                dq_t = dq_t + dotf(qkv_ref[n, 1, :, rows], ds)
                out.append((o_t, dq_t))
            return tuple(out)

        zero = jnp.zeros((dim, blk), F32)
        acc = lax.fori_loop(0, i + 1, pass_three, tuple((zero, zero) for _ in range(heads)))
        for n in range(heads):
            o_ref[n, :, cols] = acc[n][0].astype(BF16)
            dqkv_ref[n, 0, :, cols] = (acc[n][1] * scale).astype(BF16)
    for n in range(heads):
        dqkv_ref[n, 1] = dk_s[n].T.astype(BF16)
        dqkv_ref[n, 2] = dv_s[n].T.astype(BF16)


def attention(qkv, grad_o):
    heads, _, dim, seq = qkv.shape
    blk = min(512, seq)
    vmem = pl.BlockSpec(memory_space=pltpu.VMEM)
    area = heads * seq * seq * dim
    return pl.pallas_call(
        functools.partial(attention_kernel, blk, heads, dim, seq),
        out_shape=(jax.ShapeDtypeStruct((heads, dim, seq), BF16), jax.ShapeDtypeStruct(qkv.shape, BF16)),
        in_specs=[vmem, vmem], out_specs=(vmem, vmem),
        scratch_shapes=[pltpu.VMEM((heads, seq, dim), BF16), pltpu.VMEM((heads, seq, dim), BF16),
                        pltpu.VMEM((heads, seq, blk), F32), pltpu.VMEM((heads, seq, blk), F32),
                        pltpu.VMEM((heads, seq, dim), F32), pltpu.VMEM((heads, seq, dim), F32)],
        compiler_params=pltpu.CompilerParams(vmem_limit_bytes=50 * 2 ** 20),
        cost_estimate=pl.CostEstimate(flops=24 * area, bytes_accessed=20 * heads * seq * dim, transcendentals=0),
        name="attention",
    )(qkv, grad_o)


MESH = pl.DeviceIdType.MESH
CHUNK = 128


def line_kernel(total, hidden, tasks_of, n_in, n_out, *refs):
    part, base_hbm, z_hbm, mu, rs, gain = refs[:6]
    task_in = refs[6:6 + n_in]
    out = refs[6 + n_in]
    task_out = refs[7 + n_in:7 + n_in + n_out]
    (pr, eb, acc, mb, base_v, z_v, mu_c, rs_c, lsem, p_snd, p_rcv, e_snd, e_rcv, m_snd, m_rcv, x_snd, x_rcv,
     y_snd, y_rcv, w_snd, w_rcv) = refs[7 + n_in + n_out:28 + n_in + n_out]
    task_scr = refs[28 + n_in + n_out:]
    half, quarter = total // 2, total // 4
    nk = quarter // CHUNK
    t = lax.axis_index('tp')
    c, z = lax.rem(t, 2), lax.div(t, 2)
    partner = t + 1 - 2 * c
    mate = 2 * (z + 1 - 2 * lax.rem(z, 2)) + c
    other = 2 * (3 - z) + c
    near = lax.div(z, 2)
    far = 1 - near
    is_mid = jnp.logical_or(z == 1, z == 2)
    is_end = jnp.logical_not(is_mid)

    def rows(s, k):
        return pl.ds(pl.multiple_of(s * quarter + k * CHUNK, CHUNK), CHUNK)

    def grows(cc, s, k):
        return pl.ds(pl.multiple_of(cc * half + s * quarter + k * CHUNK, CHUNK), CHUNK)

    def remote(src, dst, snd, rcv, dev):
        return pltpu.make_async_remote_copy(src_ref=src, dst_ref=dst, send_sem=snd, recv_sem=rcv,
                                            device_id={'tp': dev}, device_id_type=MESH)

    def p_copy(s, k):
        return remote(part.at[grows(1 - c, s, k)], pr.at[rows(s, k)], p_snd.at[s * nk + k], p_rcv.at[s * nk + k],
                      partner)

    def e_copy(s, k):
        return remote(acc.at[rows(s, k)], eb.at[rows(s, k)], e_snd.at[s * nk + k], e_rcv.at[s * nk + k], mate)

    def m_copy(k):
        return remote(acc.at[rows(far, k)], mb.at[pl.ds(k * CHUNK, CHUNK)], m_snd.at[k], m_rcv.at[k], other)

    def x_copy(s, k):
        here = out.at[grows(c, s, k)]
        return remote(here, here, x_snd.at[k], x_rcv.at[k], other)

    def y_copy(s, k):
        here = out.at[grows(c, s, k)]
        return remote(here, here, y_snd.at[s * nk + k], y_rcv.at[s * nk + k], mate)

    def w_copy(cc, s, k):
        here = out.at[grows(cc, s, k)]
        return remote(here, here, w_snd.at[s * nk + k], w_rcv.at[s * nk + k], partner)

    barrier = pltpu.get_barrier_semaphore()
    pl.semaphore_signal(barrier, inc=1, device_id={'tp': partner}, device_id_type=MESH)
    pl.semaphore_signal(barrier, inc=1, device_id={'tp': mate}, device_id_type=MESH)

    @pl.when(is_mid)
    def _():
        pl.semaphore_signal(barrier, inc=1, device_id={'tp': other}, device_id_type=MESH)
        own = pl.ds(pl.multiple_of(c * half + near * quarter, CHUNK), quarter)
        pltpu.make_async_copy(base_hbm.at[own], base_v, lsem.at[0]).start()
        pltpu.make_async_copy(z_hbm.at[own], z_v, lsem.at[1]).start()
        pl.semaphore_wait(barrier, 3)

    @pl.when(is_end)
    def _():
        pl.semaphore_wait(barrier, 2)

    for k in range(nk):
        for s in (far, near):
            p_copy(s, k).start()

    def summed(s, k, extra, i):
        r = pl.ds(pl.multiple_of(s * quarter + k * CHUNK + i * 16, 16), 16)
        g = pl.ds(pl.multiple_of(c * half + s * quarter + k * CHUNK + i * 16, 16), 16)
        tot = part[g, :].astype(F32) + pr[r, :].astype(F32)
        if extra:
            tot = tot + eb[r, :].astype(F32)
        return r, g, tot

    def add_rows(s, k, extra):
        @pl.loop(0, CHUNK // 16)
        def _(i):
            r, _g, tot = summed(s, k, extra, i)
            acc[r, :] = tot.astype(BF16)

    def far_event(k):
        p_copy(far, k).wait_recv()
        e_copy(far, k).wait_recv()
        add_rows(far, k, True)
        m_copy(k).start()

    def near_event(k):
        p_copy(near, k).wait_recv()
        e_copy(near, k).wait_recv()
        m_copy(k).wait_recv()
        if k == 0:
            pltpu.make_async_copy(base_hbm.at[pl.ds(0, quarter)], base_v, lsem.at[0]).wait()
            pltpu.make_async_copy(z_hbm.at[pl.ds(0, quarter)], z_v, lsem.at[1]).wait()
        stat = c * (half // CHUNK) + near * nk + k
        mu_c[...] = jnp.broadcast_to(mu[pl.ds(stat, 1), :], (CHUNK, CHUNK)).T
        rs_c[...] = jnp.broadcast_to(rs[pl.ds(stat, 1), :], (CHUNK, CHUNK)).T

        @pl.loop(0, CHUNK // 16)
        def _(i):
            _r, g, tot = summed(near, k, True, i)
            q = pl.ds(pl.multiple_of(k * CHUNK + i * 16, 16), 16)
            sub = pl.ds(pl.multiple_of(i * 16, 16), 16)
            u = (tot + mb[q, :].astype(F32)) * gain[...]
            r_col = rs_c[sub, :1]
            zhat = (z_v[q, :].astype(F32) - mu_c[sub, :1]) * r_col
            mean_u = jnp.sum(u, axis=1, keepdims=True) * (1.0 / hidden)
            mean_c = jnp.sum(u * zhat, axis=1, keepdims=True) * (1.0 / hidden)
            out[g, :] = (base_v[q, :].astype(F32) + r_col * (u - mean_u - zhat * mean_c)).astype(BF16)

        y_copy(near, k).start()
        x_copy(near, k).start()
        w_copy(c, near, k).start()

    def forward_event(k):
        x_copy(far, k).wait_recv()
        y_copy(far, k).start()
        w_copy(c, far, k).start()

    def end_send():
        for k in range(nk):
            for s in (far, near):
                p_copy(s, k).wait_recv()
                add_rows(s, k, False)
                e_copy(s, k).start()

    def end_relay(s, k):
        y_copy(s, k).wait_recv()
        w_copy(c, s, k).start()

    tasks = tasks_of(task_in, task_out, task_scr) if tasks_of else []
    steps = nk + 3
    share = -(-len(tasks) // steps) if tasks else 0
    for step in range(steps):
        @pl.when(is_mid)
        def _():
            if step < nk:
                far_event(step)
            if 0 <= step - 1 < nk:
                near_event(step - 1)
            if 0 <= step - 2 < nk:
                forward_event(step - 2)

        @pl.when(is_end)
        def _():
            if step == 0:
                end_send()
            if 0 <= step - 2 < nk:
                end_relay(near, step - 2)
            if 0 <= step - 3 < nk:
                end_relay(far, step - 3)

        for task in tasks[step * share:(step + 1) * share]:
            task()

    for k in range(nk):
        for s in (far, near):
            w_copy(1 - c, s, k).wait_recv()
            w_copy(c, s, k).wait_send()
            p_copy(s, k).wait_send()

    @pl.when(is_mid)
    def _():
        for k in range(nk):
            m_copy(k).wait_send()
            x_copy(near, k).wait_send()
            y_copy(near, k).wait_send()
            y_copy(far, k).wait_send()

    @pl.when(is_end)
    def _():
        for k in range(nk):
            for s in (far, near):
                e_copy(s, k).wait_send()


def line_reduce(part, base, z, mu, rs, gain, cid, tasks_of=None, task_in=(), task_out=(), task_scr=()):
    total, hidden = part.shape
    half, quarter = total // 2, total // 4
    n = half // CHUNK
    vmem = pl.BlockSpec(memory_space=pltpu.VMEM)
    hbm = pl.BlockSpec(memory_space=pl.ANY)
    sem = pltpu.SemaphoreType.DMA
    buf = pltpu.VMEM((half, hidden), BF16)
    buf_q = pltpu.VMEM((quarter, hidden), BF16)
    col = pltpu.VMEM((CHUNK, CHUNK), F32)
    outs = pl.pallas_call(
        functools.partial(line_kernel, total, hidden, tasks_of, len(task_in), len(task_out)),
        out_shape=(jax.ShapeDtypeStruct((total, hidden), BF16), *task_out),
        in_specs=[vmem, hbm, hbm, vmem, vmem, vmem] + [vmem] * len(task_in),
        out_specs=tuple([vmem] * (1 + len(task_out))),
        scratch_shapes=[buf, buf, buf, buf_q, buf_q, buf_q, col, col, sem((2,)),
                        sem((n,)), sem((n,)), sem((n,)), sem((n,)), sem((n // 2,)), sem((n // 2,)),
                        sem((n // 2,)), sem((n // 2,)), sem((n,)), sem((n,)), sem((n,)), sem((n,)), *task_scr],
        compiler_params=pltpu.CompilerParams(collective_id=cid, has_side_effects=True,
                                             vmem_limit_bytes=60 * 2 ** 20),
        name=f"line_reduce_{cid}",
    )(part, base, z, mu.reshape(total // CHUNK, CHUNK), rs.reshape(total // CHUNK, CHUNK),
      gain.astype(F32).reshape(1, hidden), *task_in)
    return outs


def solution(mesh):
    act_spec = P('dp', None, None)
    stat_spec = P('dp', None)
    in_specs = (act_spec, act_spec, act_spec, stat_spec, stat_spec, stat_spec, stat_spec, P(), P(),
                P(None, 'tp', None, None), P('tp', None, None), P(None, 'tp'), P('tp', None))
    out_specs = (act_spec, P('dp', 'tp', None, None), P(('dp', 'tp'), None, None), P('dp', 'tp'),
                 P(('dp', 'tp'), None))

    def local_backward(x_saved, h1_saved, grad_y, mean_one, rstd_one, mean_two, rstd_two,
                       gain_one, gain_two, w_qkv, w_out, w_up, w_down):
        mbs = x_saved.shape[0]
        zhat_two = (h1_saved.astype(F32) - mean_two[..., None]) * rstd_two[..., None]
        norm_two = (zhat_two * gain_two.astype(F32)).astype(BF16)
        act_out, grad_pre, part_two = [], [], []
        for b in range(mbs):
            value, slope = gelu_both(wide_einsum('sh,hf->sf', norm_two[b], w_up))
            act_out.append(value.astype(BF16))
            grad_pre.append((wide_einsum('sh,fh->sf', grad_y[b], w_down) * slope).astype(BF16))
            part_two.append(wide_einsum('sf,hf->sh', grad_pre[b], w_up).astype(BF16))
        grad_down = wide_einsum('msf,msh->fh', jnp.stack(act_out), grad_y).astype(BF16)
        grad_up = wide_einsum('msh,msf->hf', norm_two, jnp.stack(grad_pre)).astype(BF16)
        zhat_one = (x_saved.astype(F32) - mean_one[..., None]) * rstd_one[..., None]
        norm_one = (zhat_one * gain_one.astype(F32)).astype(BF16)
        grad_x, attn_out, grad_qkv, grad_h1 = [], [], [], []
        for b in range(mbs):
            dh, = line_reduce(part_two[b], grad_y[b], h1_saved[b], mean_two[b], rstd_two[b], gain_two, 2 * b)
            qkv = wide_einsum('sh,hncd->ncds', norm_one[b], w_qkv).astype(BF16)
            grad_o = wide_einsum('sh,ndh->nds', dh, w_out).astype(BF16)
            o, dqkv = attention(qkv, grad_o)
            part = wide_einsum('ncds,hncd->sh', dqkv, w_qkv).astype(BF16)
            dx, = line_reduce(part, dh, x_saved[b], mean_one[b], rstd_one[b], gain_one, 2 * b + 1)
            grad_x.append(dx)
            attn_out.append(o)
            grad_qkv.append(dqkv)
            grad_h1.append(dh)
        grad_out_w = wide_einsum('mnds,msh->ndh', jnp.stack(attn_out), jnp.stack(grad_h1)).astype(BF16)
        grad_qkv_w = wide_einsum('msh,mncds->hncd', norm_one, jnp.stack(grad_qkv)).astype(BF16)
        return jnp.stack(grad_x), grad_qkv_w, grad_out_w, grad_up, grad_down

    return jax.shard_map(local_backward, mesh=mesh, in_specs=in_specs, out_specs=out_specs, check_vma=False)
```
